8 devices in a mesh: dp: 1 (over z), cols: 2 (over y), rows: 4 (over x, core).
Axes of the slice: x: 2, y: 2, z: 1, core: 2. Of those that a mesh axis runs over, the one named last changes fastest.
Arguments:
- h_init: bfloat16 [2, 128, 48, 128], P('dp', 'rows', 'cols')
- c_init: float32 [2, 128, 48, 128], P('dp', 'rows', 'cols')
- w_rec: bfloat16 [3, 3, 128, 512], replicated
- gate_bias: float32 [24, 512], replicated
Outputs:
- output 1: bfloat16 [24, 2, 128, 48, 128], P(None, 'dp', 'rows', 'cols')
- output 2: float32 [2, 128, 48, 128], P('dp', 'rows', 'cols')
All inputs are finite; a program needn't handle non-finite values.
Results may differ from the reference program's by a relative error of at most 0.00377757.
Values are sent between devices in bfloat16 or wider.
A program may use at most 1 GiB of HBM per device.

```python
import jax
import jax.numpy as jnp
from jax import lax

STEPS = 24
BATCH = 2
GRID_H = 128
GRID_W = 48
CHANNELS = 128


def setup_inputs(seed: int = 0, part: int = 0) -> dict:
    key_w, key_b = jax.random.split(jax.random.key(seed))
    part_key = jax.random.fold_in(jax.random.key(seed + 1), part)
    key_h, key_c = jax.random.split(part_key)
    fan_in = 9 * CHANNELS
    w_rec = (jax.random.normal(key_w, (3, 3, CHANNELS, 4 * CHANNELS), jnp.float32) * (1.5 * fan_in ** -0.5)).astype(jnp.bfloat16)
    gate_offset = jnp.repeat(jnp.array([0.0, 1.0, 0.0, 0.0], jnp.float32), CHANNELS)
    gate_bias = jax.random.normal(key_b, (STEPS, 4 * CHANNELS), jnp.float32) * 0.5 + gate_offset
    h_init = (jax.random.normal(key_h, (BATCH, GRID_H, GRID_W, CHANNELS), jnp.float32) * 0.6).astype(jnp.bfloat16)
    c_init = jax.random.normal(key_c, (BATCH, GRID_H, GRID_W, CHANNELS), jnp.float32)
    return {"h_init": h_init, "c_init": c_init, "w_rec": w_rec, "gate_bias": gate_bias}


def reference(h_init, c_init, w_rec, gate_bias):
    w_wide = w_rec.astype(jnp.float32)

    def one_step(carry_in, bias_row):
        h_prev, c_prev = carry_in
        gate_pre = lax.conv_general_dilated(h_prev.astype(jnp.float32), w_wide, (1, 1), "SAME", dimension_numbers=("NHWC", "HWIO", "NHWC")) + bias_row
        in_gate, forget_gate, out_gate, cand_gate = jnp.split(gate_pre, 4, axis=-1)
        c_next = jax.nn.sigmoid(forget_gate) * c_prev + jax.nn.sigmoid(in_gate) * jnp.tanh(cand_gate)
        h_next = (jax.nn.sigmoid(out_gate) * jnp.tanh(c_next)).astype(jnp.bfloat16)
        return (h_next, c_next), h_next

    final_state, h_seq = lax.scan(one_step, (h_init, c_init), gate_bias)
    return h_seq, final_state[1]
```

```python
import jax
import jax.numpy as jnp
from jax import lax
from jax.experimental import pallas as pl
from jax.experimental.pallas import tpu as pltpu
from jax.sharding import PartitionSpec as P

MESH = pl.DeviceIdType.MESH
STEPS, BATCH, H, W, C = 24, 2, 32, 24, 128
RC = 8
NC = H // RC
M = RC * W
PITCH = 40
ROWS = H + 2


def sigmoid(x):
    return 0.5 * jnp.tanh(0.5 * x) + 0.5


def kernel(h0, c0, w, bias, hseq, clast, hxa, hxb, stage, sendcol, recvcol, recvcor, recvrow,
           s_col, r_col, s_cor, r_cor, s_row, r_row, s_out):
    hx = (hxa, hxb)
    row = lax.axis_index("rows")
    col = lax.axis_index("cols")
    nrow = lax.axis_size("rows")
    up = lax.rem(row + nrow - 1, nrow)
    down = lax.rem(row + 1, nrow)
    side = 1 - col
    dev_side = {"cols": side}
    dev_row = ({"rows": up}, {"rows": down})
    dev_cor = ({"rows": up, "cols": side}, {"rows": down, "cols": side})

    barrier = pltpu.get_barrier_semaphore()
    for dev in (dev_side,) + dev_row + dev_cor:
        pl.semaphore_signal(barrier, inc=1, device_id=dev, device_id_type=MESH)

    has = (jnp.where(row > 0, 1.0, 0.0), jnp.where(row < nrow - 1, 1.0, 0.0))
    is_left = jnp.where(col == 0, 1.0, 0.0)

    def col_copy(s, b, i):
        return pltpu.make_async_remote_copy(sendcol.at[s, b, i], recvcol.at[s, b, i], s_col.at[s, b, i], r_col.at[s, b, i],
                                            device_id=dev_side, device_id_type=MESH)

    def cor_copy(s, b, d):
        i = 0 if d == 0 else NC - 1
        return pltpu.make_async_remote_copy(sendcol.at[s, b, i], recvcor.at[s, b, 1 - d], s_cor.at[s, b, d], r_cor.at[s, b, 1 - d],
                                            device_id=dev_cor[d], device_id_type=MESH)

    def row_copy(s, b, d):
        src = 1 if d == 0 else H
        return pltpu.make_async_remote_copy(hx[s].at[b, src, 8:8 + W, :], recvrow.at[s, b, 1 - d], s_row.at[s, b, d],
                                            r_row.at[s, b, 1 - d], device_id=dev_row[d], device_id_type=MESH)

    def out_copy(s, b, t):
        return pltpu.make_async_copy(stage.at[s, b], hseq.at[t, b], s_out.at[s, b])

    def put(s, b, i, h, send):
        h3 = h.reshape(RC, W, C)
        hx[s][b, 1 + i * RC:1 + (i + 1) * RC, 8:8 + W, :] = h3
        if send:
            sendcol[s, b, i] = jnp.where(col == 0, h3[:, W - 1, :], h3[:, 0, :])
            col_copy(s, b, i).start()
            if i == 0:
                row_copy(s, b, 0).start()
                cor_copy(s, b, 0).start()
            if i == NC - 1:
                row_copy(s, b, 1).start()
                cor_copy(s, b, 1).start()

    def send_done(s, b, i):
        col_copy(s, b, i).wait_send()
        if i == 0:
            row_copy(s, b, 0).wait_send()
            cor_copy(s, b, 0).wait_send()
        if i == NC - 1:
            row_copy(s, b, 1).wait_send()
            cor_copy(s, b, 1).wait_send()

    def take_col(s, b, i):
        col_copy(s, b, i).wait_recv()
        v = recvcol[s, b, i]
        hx[s][b, 1 + i * RC:1 + (i + 1) * RC, 7, :] = v * (1.0 - is_left)
        hx[s][b, 1 + i * RC:1 + (i + 1) * RC, 8 + W, :] = v * is_left

    def take_row(s, b, d):
        r = 0 if d == 0 else H + 1
        k = RC - 1 if d == 0 else 0
        row_copy(s, b, 1 - d).wait_recv()
        cor_copy(s, b, 1 - d).wait_recv()
        hx[s][b, r, 8:8 + W, :] = recvrow[s, b, d] * has[d]
        v = recvcor[s, b, d, k:k + 1, :] * has[d]
        hx[s][b, r, 7:8, :] = v * (1.0 - is_left)
        hx[s][b, r, 8 + W:9 + W, :] = v * is_left

    def step(s, t, send, first_out):
        n = 1 - s
        bias_row = bias[pl.ds(t, 1), :]
        for b in range(BATCH):
            for i in range(NC):
                if i == 0:
                    take_col(s, b, 0)
                    take_row(s, b, 0)
                if i + 1 < NC:
                    take_col(s, b, i + 1)
                else:
                    take_row(s, b, 1)
                taps = []
                for dh in range(3):
                    for dw in range(3):
                        v = hx[s][b, i * RC + dh:(i + 1) * RC + dh, 7 + dw:7 + dw + W, :]
                        taps.append(v.reshape(M, C).astype(jnp.bfloat16))
                lhs = jnp.concatenate(taps, axis=1)
                gate = jnp.dot(lhs, w[...], preferred_element_type=jnp.float32) + bias_row
                c_prev = clast[b, i * M:(i + 1) * M, :]
                c_next = (sigmoid(gate[:, C:2 * C]) * c_prev
                          + sigmoid(gate[:, :C]) * jnp.tanh(gate[:, 3 * C:]))
                clast[b, i * M:(i + 1) * M, :] = c_next
                h = (sigmoid(gate[:, 2 * C:3 * C]) * jnp.tanh(c_next)).astype(jnp.bfloat16)
                stage[n, b, i * M:(i + 1) * M, :] = h
                send_done(s, b, i)
                put(n, b, i, h.astype(jnp.float32), send)
            if not first_out:
                out_copy(s, b, t - 1).wait()
            out_copy(n, b, t).start()

    clast[...] = c0[...]
    for s in range(2):
        for b in range(BATCH):
            hx[s][b, :, 0:8, :] = jnp.zeros((ROWS, 8, C), jnp.float32)
            hx[s][b, :, 8 + W:PITCH, :] = jnp.zeros((ROWS, PITCH - 8 - W, C), jnp.float32)
    pl.semaphore_wait(barrier, 5)
    for b in range(BATCH):
        for i in range(NC):
            put(0, b, i, h0[b, i * M:(i + 1) * M, :].astype(jnp.float32), True)

    step(0, 0, True, True)
    step(1, 1, True, False)

    def pair(p, _):
        step(0, 2 * p, True, False)
        step(1, 2 * p + 1, True, False)
        return 0

    lax.fori_loop(1, STEPS // 2 - 1, pair, 0)
    step(0, STEPS - 2, True, False)
    step(1, STEPS - 1, False, False)
    for b in range(BATCH):
        out_copy(0, b, STEPS - 1).wait()


def solution(mesh):
    def device_fn(h_init, c_init, w_rec, gate_bias):
        cells = H * W
        vm = pl.BlockSpec(memory_space=pltpu.VMEM)
        hseq, clast = pl.pallas_call(
            kernel,
            out_shape=(jax.ShapeDtypeStruct((STEPS, BATCH, cells, C), jnp.bfloat16),
                       jax.ShapeDtypeStruct((BATCH, cells, C), jnp.float32)),
            in_specs=[vm] * 4,
            out_specs=(pl.BlockSpec(memory_space=pl.ANY), vm),
            scratch_shapes=[
                pltpu.VMEM((BATCH, ROWS, PITCH, C), jnp.float32),
                pltpu.VMEM((BATCH, ROWS, PITCH, C), jnp.float32),
                pltpu.VMEM((2, BATCH, cells, C), jnp.bfloat16),
                pltpu.VMEM((2, BATCH, NC, RC, C), jnp.float32),
                pltpu.VMEM((2, BATCH, NC, RC, C), jnp.float32),
                pltpu.VMEM((2, BATCH, 2, RC, C), jnp.float32),
                pltpu.VMEM((2, BATCH, 2, W, C), jnp.float32),
                pltpu.SemaphoreType.DMA((2, BATCH, NC)),
                pltpu.SemaphoreType.DMA((2, BATCH, NC)),
                pltpu.SemaphoreType.DMA((2, BATCH, 2)),
                pltpu.SemaphoreType.DMA((2, BATCH, 2)),
                pltpu.SemaphoreType.DMA((2, BATCH, 2)),
                pltpu.SemaphoreType.DMA((2, BATCH, 2)),
                pltpu.SemaphoreType.DMA((2, BATCH)),
            ],
            compiler_params=pltpu.CompilerParams(collective_id=0, has_side_effects=True, vmem_limit_bytes=48 << 20),
        )(h_init.reshape(BATCH, cells, C), c_init.reshape(BATCH, cells, C), w_rec.reshape(9 * C, 4 * C), gate_bias)
        return hseq.reshape(STEPS, BATCH, H, W, C), clast.reshape(BATCH, H, W, C)

    state_spec = P("dp", "rows", "cols", None)
    return jax.shard_map(device_fn, mesh=mesh, in_specs=(state_spec, state_spec, P(), P()),
                         out_specs=(P(None, "dp", "rows", "cols", None), state_spec), check_vma=False)
```

```python
import jax
import jax.numpy as jnp
from jax import lax
from jax.experimental import pallas as pl
from jax.experimental.pallas import tpu as pltpu
from jax.sharding import PartitionSpec as P

MESH = pl.DeviceIdType.MESH
STEPS, BATCH, H, W, C = 24, 2, 32, 24, 128
PERIODS = STEPS // 2
RC = 8
NC = H // RC
M = RC * W
PITCH = 40
PAD = 8
ROWS = H + 2 * PAD
SP = 16
SROWS = H + 2 * SP
A_ORDER = (1, 2, 0, 3)
B_ORDER = (1, 2, 0, 3)


def sigmoid(x):
    return 0.5 * jnp.tanh(0.5 * x) + 0.5


def kernel(h0, c0, w, bias, hseq, c, ha, hb, hodd, sa, sb, crow, rsend, csend, ssend, stage,
           s_col, r_col, s_row, r_row, s_crow, r_crow, s_own, r_own, s_cor, r_cor, s_out):
    he = (ha, hb)
    st = (sa, sb)
    row = lax.axis_index("rows")
    col = lax.axis_index("cols")
    nrow = lax.axis_size("rows")
    up = lax.rem(row + nrow - 1, nrow)
    down = lax.rem(row + 1, nrow)
    side = 1 - col
    dev_side = {"cols": side}
    dev_row = ({"rows": up}, {"rows": down})
    dev_cor = ({"rows": up, "cols": side}, {"rows": down, "cols": side})

    has = (row > 0, row < nrow - 1)
    halo_w = jnp.where(col == 0, 8 + W, 7)
    edge_w = jnp.where(col == 0, 7 + W, 8)
    next_w = jnp.where(col == 0, 6 + W, 9)
    edge_c = jnp.where(col == 0, W - 1, 0)
    tap_plane = (jnp.where(col == 0, 0, 4), 3, jnp.where(col == 0, 4, 0))

    def remote(src, dst, ssem, rsem, dev):
        return pltpu.make_async_remote_copy(src, dst, ssem, rsem, device_id=dev, device_id_type=MESH)

    def col_copy(s, b, i):
        rows = pl.ds(SP + i * RC, RC)
        return [remote(st[s].at[b, 0:3, rows, :], st[s].at[b, 3:6, rows, :], s_col.at[s, b, i], r_col.at[s, b, i], dev_side)]

    def row_copies(s, b, d):
        o = 1 - d
        rows = pl.ds(PAD + H if d == 0 else PAD - 2, 2)
        srows = pl.ds(SP + H if d == 0 else SP - RC, RC)
        return [
            remote(rsend.at[s, b, d], he[s].at[b, rows, 8:8 + W, :], s_row.at[s, b, d], r_row.at[s, b, o], dev_row[d]),
            remote(csend.at[s, b, d], crow.at[s, b, o], s_crow.at[s, b, d], r_crow.at[s, b, o], dev_row[d]),
            remote(ssend.at[s, b, d, 0:1], st[s].at[b, 0:1, srows, :], s_own.at[s, b, d], r_own.at[s, b, o], dev_row[d]),
            remote(ssend.at[s, b, d], st[s].at[b, 3:6, srows, :], s_cor.at[s, b, d], r_cor.at[s, b, o], dev_cor[d]),
        ]

    def flat(ref, b):
        return ref.at[b].reshape(ROWS * PITCH, C)

    def strided(start, stride):
        return pl.ds(start, RC, stride)

    def out_copy(k, b, t):
        return pltpu.make_async_copy(stage.at[k, b], hseq.at[t, b], s_out.at[k, b])

    def put(s, b, i, h3, c2, send):
        he[s][b, PAD + i * RC:PAD + (i + 1) * RC, 8:8 + W, :] = h3
        if not send:
            return
        f = flat(he[s], b)
        base = (PAD + i * RC) * PITCH
        strip = (f[strided(base + edge_w, PITCH), :], f[strided(base + next_w, PITCH), :],
                 c.at[b][strided(i * M + edge_c, W), :])
        for k in range(3):
            st[s][b, k, SP + i * RC:SP + (i + 1) * RC, :] = strip[k]
        col_copy(s, b, i)[0].start()
        for d in range(2):
            if i == (0 if d == 0 else NC - 1):
                r = 0 if d == 0 else RC - 2
                q = 0 if d == 0 else (RC - 1) * W
                rsend[s, b, d] = jnp.where(has[d], h3[r:r + 2], 0.0)
                csend[s, b, d] = jnp.where(has[d], c2[q:q + W], 0.0)
                for k in range(3):
                    ssend[s, b, d, k] = jnp.where(has[d], strip[k], 0.0)
                for cp in row_copies(s, b, d):
                    cp.start()

    def insert(s, b, i):
        flat(he[s], b)[strided((PAD + i * RC) * PITCH + halo_w, PITCH), :] = st[s][b, 3, SP + i * RC:SP + (i + 1) * RC, :]

    def take_col(s, b, i):
        cp = col_copy(s, b, i)[0]
        cp.wait_send()
        cp.wait_recv()
        insert(s, b, i)

    def take_row(s, b, d):
        for cp in row_copies(s, b, d):
            cp.wait_send()
        for cp in row_copies(s, b, 1 - d):
            cp.wait_recv()
        insert(s, b, -1 if d == 0 else NC)

    def gates(parts, t):
        lhs = jnp.concatenate(parts, axis=1)
        return jnp.dot(lhs, w[...], preferred_element_type=jnp.float32)

    def update(gate, t, c_prev):
        gate = gate + bias[pl.ds(t, 1), :]
        c_next = sigmoid(gate[:, C:2 * C]) * c_prev + sigmoid(gate[:, :C]) * jnp.tanh(gate[:, 3 * C:])
        return (sigmoid(gate[:, 2 * C:3 * C]) * jnp.tanh(c_next)).astype(jnp.bfloat16), c_next

    def unit_a(s, b, i, t, seen):
        lo = i * RC - (1 if i == 0 else 0)
        n = RC + (1 if i in (0, NC - 1) else 0)
        wlo = i * RC - (RC if i == 0 else 0)
        wn = RC * (2 if i in (0, NC - 1) else 1)

        def dot():
            for j in range(max(i - 1, 0), min(i + 2, NC)):
                if j not in seen:
                    seen.add(j)
                    take_col(s, b, j)
            if i == 0:
                take_row(s, b, 0)
            if i == NC - 1:
                take_row(s, b, 1)
            parts = []
            for dh in range(3):
                for dw in range(3):
                    v = he[s][b, PAD + lo + dh - 1:PAD + lo + dh - 1 + n, 7 + dw:7 + dw + W, :].reshape(n * W, C)
                    r = st[s][b, tap_plane[dw], SP + wlo + dh - 1:SP + wlo + dh - 1 + wn, :]
                    v = jnp.concatenate([v, r, jnp.zeros((8, C), jnp.float32)], axis=0)
                    parts.append(v.astype(jnp.bfloat16))
            return gates(parts, t)

        def epilogue(gate):
            cm = c[b, i * M:(i + 1) * M, :]
            cw = st[s][b, 5, SP + wlo:SP + wlo + wn, :]
            z = jnp.zeros((8, C), jnp.float32)
            if i == 0:
                parts, m0 = [crow[s, b, 0], cm, cw, z], W
            elif i == NC - 1:
                parts, m0 = [cm, crow[s, b, 1], cw, z], 0
            else:
                parts, m0 = [cm, cw, z], 0
            h, c_next = update(gate, t, jnp.concatenate(parts, axis=0))
            c[b, i * M:(i + 1) * M, :] = c_next[m0:m0 + M]
            hf = h.astype(jnp.float32)
            main = hf[m0:m0 + M]
            stage[0, b, i * M:(i + 1) * M, :] = main.astype(jnp.bfloat16)
            hodd[b, PAD + i * RC:PAD + (i + 1) * RC, 8:8 + W, :] = main.reshape(RC, W, C)
            ring = hf[n * W:n * W + wn]
            f = flat(hodd, b)
            if i == 0:
                hodd[b, PAD - 1, 8:8 + W, :] = jnp.where(has[0], hf[:W], 0.0)
                f[strided(halo_w, PITCH), :] = jnp.where(has[0], ring[:RC], 0.0)
                f[strided(PAD * PITCH + halo_w, PITCH), :] = ring[RC:]
            elif i == NC - 1:
                hodd[b, PAD + H, 8:8 + W, :] = jnp.where(has[1], hf[M:M + W], 0.0)
                f[strided((PAD + i * RC) * PITCH + halo_w, PITCH), :] = ring[:RC]
                f[strided((PAD + H) * PITCH + halo_w, PITCH), :] = jnp.where(has[1], ring[RC:], 0.0)
            else:
                f[strided((PAD + i * RC) * PITCH + halo_w, PITCH), :] = ring

        return dot, epilogue

    def unit_b(n, b, i, t, send):
        def dot():
            parts = []
            for dh in range(3):
                for dw in range(3):
                    v = hodd[b, PAD + i * RC + dh - 1:PAD + (i + 1) * RC + dh - 1, 7 + dw:7 + dw + W, :]
                    parts.append(v.reshape(M, C).astype(jnp.bfloat16))
            return gates(parts, t)

        def epilogue(gate):
            h, c_next = update(gate, t, c[b, i * M:(i + 1) * M, :])
            c[b, i * M:(i + 1) * M, :] = c_next
            stage[1, b, i * M:(i + 1) * M, :] = h
            put(n, b, i, h.astype(jnp.float32).reshape(RC, W, C), c_next, send)

        return dot, epilogue

    def period(s, p, send):
        t = 2 * p
        n = 1 - s
        units = []
        for b in range(BATCH):
            seen = set()
            for i in A_ORDER:
                units.append((unit_a(s, b, i, t, seen), (0, b, t) if i == A_ORDER[-1] else None))
            for i in B_ORDER:
                units.append((unit_b(n, b, i, t + 1, send), (1, b, t + 1) if i == B_ORDER[-1] else None))
        held = None
        for unit in units + [None]:
            gate = unit[0][0]() if unit else None
            if held:
                (_, epilogue), out = held[0]
                epilogue(held[1])
                if out:
                    k, b, tt = out
                    out_copy(k, b, tt).start()
                    if k == 1:
                        out_copy(0, b, tt - 1).wait()
                        if b == 1:
                            out_copy(1, 0, tt).wait()
            held = (unit, gate) if unit else None

    c[...] = c0[...]
    for b in range(BATCH):
        for ref in (ha, hb, hodd):
            for at in (0, 8 + W):
                ref[b, :, at:at + 8, :] = jnp.zeros((ROWS, 8, C), jnp.float32)
    barrier = pltpu.get_barrier_semaphore()
    for dev in (dev_side,) + dev_row + dev_cor:
        pl.semaphore_signal(barrier, inc=1, device_id=dev, device_id_type=MESH)
    pl.semaphore_wait(barrier, 5)
    for b in range(BATCH):
        for i in range(NC):
            h = h0[b, i * M:(i + 1) * M, :].astype(jnp.float32).reshape(RC, W, C)
            put(0, b, i, h, c[b, i * M:(i + 1) * M, :], True)

    def two(q, _):
        @pl.when(q > 0)
        def _():
            out_copy(1, 1, 4 * q - 1).wait()
        period(0, 2 * q, True)
        out_copy(1, 1, 4 * q + 1).wait()
        period(1, 2 * q + 1, True)
        return 0

    lax.fori_loop(0, PERIODS // 2 - 1, two, 0)
    out_copy(1, 1, STEPS - 5).wait()
    period(0, PERIODS - 2, True)
    out_copy(1, 1, STEPS - 3).wait()
    period(1, PERIODS - 1, False)
    out_copy(1, 1, STEPS - 1).wait()


def solution(mesh):
    def device_fn(h_init, c_init, w_rec, gate_bias):
        cells = H * W
        vm = pl.BlockSpec(memory_space=pltpu.VMEM)
        tile = pltpu.VMEM((BATCH, ROWS, PITCH, C), jnp.float32)
        strip = pltpu.VMEM((BATCH, 6, SROWS, C), jnp.float32)
        pair_sems = pltpu.SemaphoreType.DMA((2, BATCH, 2))
        hseq, clast = pl.pallas_call(
            kernel,
            out_shape=(jax.ShapeDtypeStruct((STEPS, BATCH, cells, C), jnp.bfloat16),
                       jax.ShapeDtypeStruct((BATCH, cells, C), jnp.float32)),
            in_specs=[vm] * 4,
            out_specs=(pl.BlockSpec(memory_space=pl.ANY), vm),
            scratch_shapes=[
                tile, tile, tile, strip, strip,
                pltpu.VMEM((2, BATCH, 2, W, C), jnp.float32),
                pltpu.VMEM((2, BATCH, 2, 2, W, C), jnp.float32),
                pltpu.VMEM((2, BATCH, 2, W, C), jnp.float32),
                pltpu.VMEM((2, BATCH, 2, 3, RC, C), jnp.float32),
                pltpu.VMEM((2, BATCH, cells, C), jnp.bfloat16),
                pltpu.SemaphoreType.DMA((2, BATCH, NC)),
                pltpu.SemaphoreType.DMA((2, BATCH, NC)),
            ] + [pair_sems] * 8 + [pltpu.SemaphoreType.DMA((2, BATCH))],
            compiler_params=pltpu.CompilerParams(collective_id=0, has_side_effects=True, vmem_limit_bytes=48 << 20),
        )(h_init.reshape(BATCH, cells, C), c_init.reshape(BATCH, cells, C), w_rec.reshape(9 * C, 4 * C), gate_bias)
        return hseq.reshape(STEPS, BATCH, H, W, C), clast.reshape(BATCH, H, W, C)

    state_spec = P("dp", "rows", "cols", None)
    return jax.shard_map(device_fn, mesh=mesh, in_specs=(state_spec, state_spec, P(), P()),
                         out_specs=(P(None, "dp", "rows", "cols", None), state_spec), check_vma=False)
```

```python
import jax
import jax.numpy as jnp
from jax import lax
from jax.experimental import pallas as pl
from jax.experimental.pallas import tpu as pltpu
from jax.sharding import PartitionSpec as P

MESH = pl.DeviceIdType.MESH
STEPS, BATCH, H, W, C = 24, 2, 32, 24, 128
PERIODS = STEPS // 2
RC = 8
NC = H // RC
M = RC * W
PITCH = 40
PAD = 8
ROWS = H + 2 * PAD
SP = 16
SROWS = H + 2 * SP
PIECES = 12
A_ORDER = (1, 2, 0, 3)
B_ORDER = (0, 3, 1, 2)


def sigmoid(x):
    return 0.5 * jnp.tanh(0.5 * x) + 0.5


def kernel(h0, c0, w, bias_in, hseq, c, ha, hb, hodd, sa, sb, crow, rsend, csend, ssend, wt, hin, bias,
           s_col, r_col, s_row, r_row, s_crow, r_crow, s_own, r_own, s_cor, r_cor, s_w):
    he = (ha, hb)
    st = (sa, sb)
    row = lax.axis_index("rows")
    col = lax.axis_index("cols")
    nrow = lax.axis_size("rows")
    up = lax.rem(row + nrow - 1, nrow)
    down = lax.rem(row + 1, nrow)
    side = 1 - col
    dev_side = {"cols": side}
    dev_row = ({"rows": up}, {"rows": down})
    dev_cor = ({"rows": up, "cols": side}, {"rows": down, "cols": side})

    has = (row > 0, row < nrow - 1)
    halo_w = jnp.where(col == 0, 8 + W, 7)
    edge_w = jnp.where(col == 0, 7 + W, 8)
    next_w = jnp.where(col == 0, 6 + W, 9)
    edge_c = jnp.where(col == 0, W - 1, 0)
    tap_plane = (jnp.where(col == 0, 0, 4), 3, jnp.where(col == 0, 4, 0))

    def remote(src, dst, ssem, rsem, dev):
        return pltpu.make_async_remote_copy(src, dst, ssem, rsem, device_id=dev, device_id_type=MESH)

    def col_copy(s, b, i):
        rows = pl.ds(SP + i * RC, RC)
        return [remote(st[s].at[b, 0:3, rows, :], st[s].at[b, 3:6, rows, :], s_col.at[s, b, i], r_col.at[s, b, i], dev_side)]

    def row_copies(s, b, d):
        o = 1 - d
        rows = pl.ds(PAD + H if d == 0 else PAD - 2, 2)
        srows = pl.ds(SP + H if d == 0 else SP - RC, RC)
        return [
            remote(rsend.at[s, b, d], he[s].at[b, rows, 8:8 + W, :], s_row.at[s, b, d], r_row.at[s, b, o], dev_row[d]),
            remote(csend.at[s, b, d], crow.at[s, b, o], s_crow.at[s, b, d], r_crow.at[s, b, o], dev_row[d]),
            remote(ssend.at[s, b, d, 0:1], st[s].at[b, 0:1, srows, :], s_own.at[s, b, d], r_own.at[s, b, o], dev_row[d]),
            remote(ssend.at[s, b, d], st[s].at[b, 3:6, srows, :], s_cor.at[s, b, d], r_cor.at[s, b, o], dev_cor[d]),
        ]

    def flat(ref, b):
        return ref.at[b].reshape(ROWS * PITCH, C)

    def strided(start, stride):
        return pl.ds(start, RC, stride)

    def put(s, b, i, h3, c2, send):
        he[s][b, PAD + i * RC:PAD + (i + 1) * RC, 8:8 + W, :] = h3
        if not send:
            return
        f = flat(he[s], b)
        base = (PAD + i * RC) * PITCH
        strip = (f[strided(base + edge_w, PITCH), :], f[strided(base + next_w, PITCH), :],
                 c.at[b][strided(i * M + edge_c, W), :])
        for k in range(3):
            st[s][b, k, SP + i * RC:SP + (i + 1) * RC, :] = strip[k]
        col_copy(s, b, i)[0].start()
        for d in range(2):
            if i == (0 if d == 0 else NC - 1):
                r = 0 if d == 0 else RC - 2
                q = 0 if d == 0 else (RC - 1) * W
                rsend[s, b, d] = jnp.where(has[d], h3[r:r + 2], 0.0)
                csend[s, b, d] = jnp.where(has[d], c2[q:q + W], 0.0)
                for k in range(3):
                    ssend[s, b, d, k] = jnp.where(has[d], strip[k], 0.0)
                for cp in row_copies(s, b, d):
                    cp.start()

    def insert(s, b, i):
        flat(he[s], b)[strided((PAD + i * RC) * PITCH + halo_w, PITCH), :] = st[s][b, 3, SP + i * RC:SP + (i + 1) * RC, :]

    def take_col(s, b, i):
        cp = col_copy(s, b, i)[0]
        cp.wait_send()
        cp.wait_recv()
        insert(s, b, i)

    def take_row(s, b, d):
        for cp in row_copies(s, b, d):
            cp.wait_send()
        for cp in row_copies(s, b, 1 - d):
            cp.wait_recv()
        insert(s, b, -1 if d == 0 else NC)

    def gates(parts, t):
        lhs = jnp.concatenate(parts, axis=1)
        rhs = jnp.concatenate([wt[k] for k in range(4)], axis=1)
        return jnp.dot(lhs, rhs, preferred_element_type=jnp.float32)

    def update(gate, t, c_prev):
        gate = bias[pl.ds(t, 1), :] + gate
        c_next = sigmoid(gate[:, C:2 * C]) * c_prev + sigmoid(gate[:, :C]) * jnp.tanh(gate[:, 3 * C:])
        return (sigmoid(gate[:, 2 * C:3 * C]) * jnp.tanh(c_next)).astype(jnp.bfloat16), c_next

    def unit_a(s, b, i, t, seen):
        lo = i * RC - (1 if i == 0 else 0)
        n = RC + (1 if i in (0, NC - 1) else 0)
        wlo = i * RC - (RC if i == 0 else 0)
        wn = RC * (2 if i in (0, NC - 1) else 1)

        def dot():
            if not seen:
                seen.add(i)
                for j in range(NC):
                    take_col(s, b, j)
                for d in range(2):
                    take_row(s, b, d)
            parts = []
            for dh in range(3):
                for dw in range(3):
                    v = he[s][b, PAD + lo + dh - 1:PAD + lo + dh - 1 + n, 7 + dw:7 + dw + W, :].reshape(n * W, C)
                    r = st[s][b, tap_plane[dw], SP + wlo + dh - 1:SP + wlo + dh - 1 + wn, :]
                    v = jnp.concatenate([v, r, jnp.zeros((8, C), jnp.float32)], axis=0)
                    parts.append(v.astype(jnp.bfloat16))
            return gates(parts, t)

        def epilogue(gate):
            cm = c[b, i * M:(i + 1) * M, :]
            cw = st[s][b, 5, SP + wlo:SP + wlo + wn, :]
            z = jnp.zeros((8, C), jnp.float32)
            if i == 0:
                parts, m0 = [crow[s, b, 0], cm, cw, z], W
            elif i == NC - 1:
                parts, m0 = [cm, crow[s, b, 1], cw, z], 0
            else:
                parts, m0 = [cm, cw, z], 0
            h, c_next = update(gate, t, jnp.concatenate(parts, axis=0))
            c[b, i * M:(i + 1) * M, :] = c_next[m0:m0 + M]
            hf = h.astype(jnp.float32)
            main = hf[m0:m0 + M]
            hseq[t, b, i * M:(i + 1) * M, :] = main.astype(jnp.bfloat16)
            hodd[b, PAD + i * RC:PAD + (i + 1) * RC, 8:8 + W, :] = main.reshape(RC, W, C)
            ring = hf[n * W:n * W + wn]
            f = flat(hodd, b)
            if i == 0:
                hodd[b, PAD - 1, 8:8 + W, :] = jnp.where(has[0], hf[:W], 0.0)
                f[strided(halo_w, PITCH), :] = jnp.where(has[0], ring[:RC], 0.0)
                f[strided(PAD * PITCH + halo_w, PITCH), :] = ring[RC:]
            elif i == NC - 1:
                hodd[b, PAD + H, 8:8 + W, :] = jnp.where(has[1], hf[M:M + W], 0.0)
                f[strided((PAD + i * RC) * PITCH + halo_w, PITCH), :] = ring[:RC]
                f[strided((PAD + H) * PITCH + halo_w, PITCH), :] = jnp.where(has[1], ring[RC:], 0.0)
            else:
                f[strided((PAD + i * RC) * PITCH + halo_w, PITCH), :] = ring

        return dot, epilogue

    def unit_b(n, b, i, t, send):
        def dot():
            parts = []
            for dh in range(3):
                for dw in range(3):
                    v = hodd[b, PAD + i * RC + dh - 1:PAD + (i + 1) * RC + dh - 1, 7 + dw:7 + dw + W, :]
                    parts.append(v.reshape(M, C).astype(jnp.bfloat16))
            return gates(parts, t)

        def epilogue(gate):
            h, c_next = update(gate, t, c[b, i * M:(i + 1) * M, :])
            c[b, i * M:(i + 1) * M, :] = c_next
            hseq[t, b, i * M:(i + 1) * M, :] = h
            put(n, b, i, h.astype(jnp.float32).reshape(RC, W, C), c_next, send)

        return dot, epilogue

    def period(s, p, send):
        t = 2 * p
        n = 1 - s
        units = []
        for b in range(BATCH):
            seen = set()
            for i in A_ORDER:
                units.append(unit_a(s, b, i, t, seen))
            for i in B_ORDER:
                units.append(unit_b(n, b, i, t + 1, send))
        half = len(units) // BATCH
        for b in range(BATCH):
            held = None
            for unit in units[b * half:(b + 1) * half] + [None]:
                gate = unit[0]() if unit else None
                if held:
                    held[0][1](held[1])
                held = (unit, gate) if unit else None

    load_state = [pltpu.make_async_copy(h0, hin, s_w.at[4]), pltpu.make_async_copy(c0, c, s_w.at[5])]
    load_w = [pltpu.make_async_copy(w.at[:, k * C:(k + 1) * C], wt.at[k], s_w.at[k]) for k in range(4)]
    load_w.append(pltpu.make_async_copy(bias_in, bias, s_w.at[6]))
    for cp in load_state + load_w:
        cp.start()
    for b in range(BATCH):
        for ref in (ha, hb, hodd):
            for at in (0, 8 + W):
                ref[b, :, at:at + 8, :] = jnp.zeros((ROWS, 8, C), jnp.float32)
    barrier = pltpu.get_barrier_semaphore()
    for dev in (dev_side,) + dev_row + dev_cor:
        pl.semaphore_signal(barrier, inc=1, device_id=dev, device_id_type=MESH)
    for cp in load_state:
        cp.wait()
    pl.semaphore_wait(barrier, 5)
    for b in range(BATCH):
        for i in range(NC):
            h = hin[b, i * M:(i + 1) * M, :].astype(jnp.float32).reshape(RC, W, C)
            put(0, b, i, h, c[b, i * M:(i + 1) * M, :], True)
    for cp in load_w:
        cp.wait()

    def two(q, _):
        period(0, 2 * q, True)
        period(1, 2 * q + 1, True)
        return 0

    lax.fori_loop(0, PERIODS // 2 - 1, two, 0)
    period(0, PERIODS - 2, True)
    period(1, PERIODS - 1, False)


def write_out(h, c, h_out, c_out, sems):
    n = STEPS // PIECES
    copies = [pltpu.make_async_copy(h.at[k * n:(k + 1) * n], h_out.at[k * n:(k + 1) * n], sems.at[k]) for k in range(PIECES)]
    copies.append(pltpu.make_async_copy(c, c_out, sems.at[PIECES]))
    for cp in copies:
        cp.start()
    for cp in copies:
        cp.wait()


def solution(mesh):
    def device_fn(h_init, c_init, w_rec, gate_bias):
        cells = H * W
        vm = pl.BlockSpec(memory_space=pltpu.VMEM)
        hbm = pl.BlockSpec(memory_space=pltpu.HBM)
        tile = pltpu.VMEM((BATCH, ROWS, PITCH, C), jnp.float32)
        strip = pltpu.VMEM((BATCH, 6, SROWS, C), jnp.float32)
        pair_sems = pltpu.SemaphoreType.DMA((2, BATCH, 2))
        hseq, clast = pl.pallas_call(
            kernel,
            out_shape=(jax.ShapeDtypeStruct((STEPS, BATCH, cells, C), jnp.bfloat16),
                       jax.ShapeDtypeStruct((BATCH, cells, C), jnp.float32)),
            in_specs=[hbm, hbm, hbm, hbm],
            out_specs=(vm, vm),
            scratch_shapes=[
                tile, tile, tile, strip, strip,
                pltpu.VMEM((2, BATCH, 2, W, C), jnp.float32),
                pltpu.VMEM((2, BATCH, 2, 2, W, C), jnp.float32),
                pltpu.VMEM((2, BATCH, 2, W, C), jnp.float32),
                pltpu.VMEM((2, BATCH, 2, 3, RC, C), jnp.float32),
                pltpu.VMEM((4, 9 * C, C), jnp.bfloat16),
                pltpu.VMEM((BATCH, cells, C), jnp.bfloat16),
                pltpu.VMEM((STEPS, 4 * C), jnp.float32),
                pltpu.SemaphoreType.DMA((2, BATCH, NC)),
                pltpu.SemaphoreType.DMA((2, BATCH, NC)),
            ] + [pair_sems] * 8 + [pltpu.SemaphoreType.DMA((7,))],
            compiler_params=pltpu.CompilerParams(collective_id=0, has_side_effects=True, vmem_limit_bytes=26 << 20),
        )(*(pltpu.with_memory_space_constraint(v, pltpu.HBM) for v in (
            h_init.reshape(BATCH, cells, C), c_init.reshape(BATCH, cells, C), w_rec.reshape(9 * C, 4 * C), gate_bias)))
        anywhere = pl.BlockSpec(memory_space=pl.ANY)
        hseq, clast = pl.pallas_call(
            write_out,
            out_shape=(jax.ShapeDtypeStruct((STEPS, BATCH, cells, C), jnp.bfloat16),
                       jax.ShapeDtypeStruct((BATCH, cells, C), jnp.float32)),
            in_specs=[vm, vm],
            out_specs=(anywhere, anywhere),
            scratch_shapes=[pltpu.SemaphoreType.DMA((PIECES + 1,))],
            compiler_params=pltpu.CompilerParams(vmem_limit_bytes=26 << 20),
        )(hseq, clast)
        return hseq.reshape(STEPS, BATCH, H, W, C), clast.reshape(BATCH, H, W, C)

    state_spec = P("dp", "rows", "cols", None)
    return jax.shard_map(device_fn, mesh=mesh, in_specs=(state_spec, state_spec, P(), P()),
                         out_specs=(P(None, "dp", "rows", "cols", None), state_spec), check_vma=False)
```

```python
import jax
import jax.numpy as jnp
from jax import lax
from jax.experimental import pallas as pl
from jax.experimental.pallas import tpu as pltpu
from jax.sharding import PartitionSpec as P

MESH = pl.DeviceIdType.MESH
STEPS, BATCH, H, W, C = 24, 2, 32, 24, 128
PERIODS = STEPS // 2
RC = 8
NC = H // RC
M = RC * W
PITCH = 40
PAD = 8
ROWS = H + 2 * PAD
SP = 16
SROWS = H + 2 * SP
PACK = 3 * W + 8
CORNER = slice(3 * W, PACK)
PIECES = 12
A_ORDER = (1, 2, 0, 3)
B_ORDER = (0, 3, 1, 2)


def sigmoid(x):
    return 0.5 * jnp.tanh(0.5 * x) + 0.5


def kernel(h0, c0, w, bias_in, hseq, c, ha, hb, hodd, sa, sb, psend, precv, wt, hin, bias,
           s_col, r_col, s_row, r_row, s_w):
    he = (ha, hb)
    st = (sa, sb)
    row = lax.axis_index("rows")
    col = lax.axis_index("cols")
    nrow = lax.axis_size("rows")
    up = lax.rem(row + nrow - 1, nrow)
    down = lax.rem(row + 1, nrow)
    side = 1 - col
    dev_side = {"cols": side}
    dev_row = ({"rows": up}, {"rows": down})
    dev_cor = ({"rows": up, "cols": side}, {"rows": down, "cols": side})

    has = (row > 0, row < nrow - 1)
    halo_w = jnp.where(col == 0, 8 + W, 7)
    edge_w = jnp.where(col == 0, 7 + W, 8)
    next_w = jnp.where(col == 0, 6 + W, 9)
    edge_c = jnp.where(col == 0, W - 1, 0)
    tap_plane = (jnp.where(col == 0, 0, 4), 3, jnp.where(col == 0, 4, 0))

    def remote(src, dst, ssem, rsem, dev):
        return pltpu.make_async_remote_copy(src, dst, ssem, rsem, device_id=dev, device_id_type=MESH)

    def col_copy(s, b, lo, n):
        rows = pl.ds(SP + lo, n)
        return remote(st[s].at[b, 0:3, rows, :], st[s].at[b, 3:6, rows, :], s_col.at[s, b], r_col.at[s, b], dev_side)

    def row_copy(s, b, d, part, dev):
        return remote(psend.at[s, b, d, part], precv.at[s, b, 1 - d, part], s_row.at[s, b, d], r_row.at[s, b, 1 - d], dev)

    def row_copies(s, b, d):
        return row_copy(s, b, d, CORNER, dev_cor[d]), row_copy(s, b, d, slice(0, 3 * W), dev_row[d])

    def flat(ref, b):
        return ref.at[b].reshape(ROWS * PITCH, C)

    def strided(start, stride):
        return pl.ds(start, RC, stride)

    def put(s, b, i, h3, c2, send):
        he[s][b, PAD + i * RC:PAD + (i + 1) * RC, 8:8 + W, :] = h3
        if not send:
            return
        f = flat(he[s], b)
        base = (PAD + i * RC) * PITCH
        strip = (f[strided(base + edge_w, PITCH), :], f[strided(base + next_w, PITCH), :],
                 c.at[b][strided(i * M + edge_c, W), :])
        for k in range(3):
            st[s][b, k, SP + i * RC:SP + (i + 1) * RC, :] = strip[k]
        for d in range(2):
            if i == (0 if d == 0 else NC - 1):
                r = 0 if d == 0 else RC - 2
                q = 0 if d == 0 else (RC - 1) * W
                for k in range(3):
                    psend[s, b, d, 3 * W + 2 * k:3 * W + 2 * k + 2, :] = jnp.where(has[d], strip[k][r:r + 2], 0.0)
                psend[s, b, d, 0:2 * W, :] = jnp.where(has[d], h3[r:r + 2].reshape(2 * W, C), 0.0)
                psend[s, b, d, 2 * W:3 * W, :] = jnp.where(has[d], c2[q:q + W], 0.0)
                for cp in row_copies(s, b, d):
                    cp.start()
        col_copy(s, b, i * RC, RC).start()

    def insert(s, b, i):
        flat(he[s], b)[strided((PAD + i * RC) * PITCH + halo_w, PITCH), :] = st[s][b, 3, SP + i * RC:SP + (i + 1) * RC, :]

    def take_cols(s, b):
        cp = col_copy(s, b, 0, H)
        cp.wait_send()
        cp.wait_recv()
        for i in range(NC):
            insert(s, b, i)

    def take_row(s, b, d):
        row_copy(s, b, d, slice(0, PACK), dev_row[d]).wait_send()
        row_copy(s, b, 1 - d, slice(0, PACK), dev_row[d]).wait_recv()
        r = -2 if d == 0 else H
        he[s][b, PAD + r:PAD + r + 2, 8:8 + W, :] = precv[s, b, d, 0:2 * W, :].reshape(2, W, C)
        for k in range(3):
            st[s][b, 3 + k, SP + r:SP + r + 2, :] = precv[s, b, d, 3 * W + 2 * k:3 * W + 2 * k + 2, :]
        i = -1 if d == 0 else NC
        insert(s, b, i)
        st[s][b, 0, SP + i * RC:SP + (i + 1) * RC, :] = flat(he[s], b)[strided((PAD + i * RC) * PITCH + edge_w, PITCH), :]

    def gates(parts, t):
        lhs = jnp.concatenate(parts, axis=1)
        rhs = jnp.concatenate([wt[k] for k in range(4)], axis=1)
        return jnp.dot(lhs, rhs, preferred_element_type=jnp.float32)

    def update(gate, t, c_prev):
        gate = bias[pl.ds(t, 1), :] + gate
        c_next = sigmoid(gate[:, C:2 * C]) * c_prev + sigmoid(gate[:, :C]) * jnp.tanh(gate[:, 3 * C:])
        return (sigmoid(gate[:, 2 * C:3 * C]) * jnp.tanh(c_next)).astype(jnp.bfloat16), c_next

    def unit_a(s, b, i, t, seen):
        lo = i * RC - (1 if i == 0 else 0)
        n = RC + (1 if i in (0, NC - 1) else 0)
        wlo = i * RC - (RC if i == 0 else 0)
        wn = RC * (2 if i in (0, NC - 1) else 1)

        def dot():
            if not seen:
                seen.add(i)
                take_cols(s, b)
                for d in range(2):
                    take_row(s, b, d)
            parts = []
            for dh in range(3):
                for dw in range(3):
                    v = he[s][b, PAD + lo + dh - 1:PAD + lo + dh - 1 + n, 7 + dw:7 + dw + W, :].reshape(n * W, C)
                    r = st[s][b, tap_plane[dw], SP + wlo + dh - 1:SP + wlo + dh - 1 + wn, :]
                    v = jnp.concatenate([v, r, jnp.zeros((8, C), jnp.float32)], axis=0)
                    parts.append(v.astype(jnp.bfloat16))
            return gates(parts, t)

        def epilogue(gate):
            cm = c[b, i * M:(i + 1) * M, :]
            cw = st[s][b, 5, SP + wlo:SP + wlo + wn, :]
            z = jnp.zeros((8, C), jnp.float32)
            if i == 0:
                parts, m0 = [precv[s, b, 0, 2 * W:3 * W, :], cm, cw, z], W
            elif i == NC - 1:
                parts, m0 = [cm, precv[s, b, 1, 2 * W:3 * W, :], cw, z], 0
            else:
                parts, m0 = [cm, cw, z], 0
            h, c_next = update(gate, t, jnp.concatenate(parts, axis=0))
            c[b, i * M:(i + 1) * M, :] = c_next[m0:m0 + M]
            hf = h.astype(jnp.float32)
            main = hf[m0:m0 + M]
            hseq[t, b, i * M:(i + 1) * M, :] = main.astype(jnp.bfloat16)
            hodd[b, PAD + i * RC:PAD + (i + 1) * RC, 8:8 + W, :] = main.reshape(RC, W, C)
            ring = hf[n * W:n * W + wn]
            f = flat(hodd, b)
            if i == 0:
                hodd[b, PAD - 1, 8:8 + W, :] = jnp.where(has[0], hf[:W], 0.0)
                f[strided(halo_w, PITCH), :] = jnp.where(has[0], ring[:RC], 0.0)
                f[strided(PAD * PITCH + halo_w, PITCH), :] = ring[RC:]
            elif i == NC - 1:
                hodd[b, PAD + H, 8:8 + W, :] = jnp.where(has[1], hf[M:M + W], 0.0)
                f[strided((PAD + i * RC) * PITCH + halo_w, PITCH), :] = ring[:RC]
                f[strided((PAD + H) * PITCH + halo_w, PITCH), :] = jnp.where(has[1], ring[RC:], 0.0)
            else:
                f[strided((PAD + i * RC) * PITCH + halo_w, PITCH), :] = ring

        return dot, epilogue

    def unit_b(n, b, i, t, send):
        def dot():
            parts = []
            for dh in range(3):
                for dw in range(3):
                    v = hodd[b, PAD + i * RC + dh - 1:PAD + (i + 1) * RC + dh - 1, 7 + dw:7 + dw + W, :]
                    parts.append(v.reshape(M, C).astype(jnp.bfloat16))
            return gates(parts, t)

        def epilogue(gate):
            h, c_next = update(gate, t, c[b, i * M:(i + 1) * M, :])
            c[b, i * M:(i + 1) * M, :] = c_next
            hseq[t, b, i * M:(i + 1) * M, :] = h
            put(n, b, i, h.astype(jnp.float32).reshape(RC, W, C), c_next, send)

        return dot, epilogue

    def period(s, p, send):
        t = 2 * p
        n = 1 - s
        units = []
        for b in range(BATCH):
            seen = set()
            for i in A_ORDER:
                units.append(unit_a(s, b, i, t, seen))
            for i in B_ORDER:
                units.append(unit_b(n, b, i, t + 1, send))
        half = len(units) // BATCH
        for b in range(BATCH):
            held = None
            for unit in units[b * half:(b + 1) * half] + [None]:
                gate = unit[0]() if unit else None
                if held:
                    held[0][1](held[1])
                held = (unit, gate) if unit else None

    load_state = [pltpu.make_async_copy(h0, hin, s_w.at[4]), pltpu.make_async_copy(c0, c, s_w.at[5])]
    load_w = [pltpu.make_async_copy(w.at[:, k * C:(k + 1) * C], wt.at[k], s_w.at[k]) for k in range(4)]
    load_w.append(pltpu.make_async_copy(bias_in, bias, s_w.at[6]))
    for cp in load_state + load_w:
        cp.start()
    for b in range(BATCH):
        for ref in (ha, hb, hodd):
            for at in (0, 8 + W):
                ref[b, :, at:at + 8, :] = jnp.zeros((ROWS, 8, C), jnp.float32)
    barrier = pltpu.get_barrier_semaphore()
    for dev in (dev_side,) + dev_row + dev_cor:
        pl.semaphore_signal(barrier, inc=1, device_id=dev, device_id_type=MESH)
    for cp in load_state:
        cp.wait()
    pl.semaphore_wait(barrier, 5)
    for b in range(BATCH):
        for i in range(NC):
            h = hin[b, i * M:(i + 1) * M, :].astype(jnp.float32).reshape(RC, W, C)
            put(0, b, i, h, c[b, i * M:(i + 1) * M, :], True)
    for cp in load_w:
        cp.wait()

    def two(q, _):
        period(0, 2 * q, True)
        period(1, 2 * q + 1, True)
        return 0

    lax.fori_loop(0, PERIODS // 2 - 1, two, 0)
    period(0, PERIODS - 2, True)
    period(1, PERIODS - 1, False)


def write_out(h, c, h_out, c_out, sems):
    n = STEPS // PIECES
    copies = [pltpu.make_async_copy(h.at[k * n:(k + 1) * n], h_out.at[k * n:(k + 1) * n], sems.at[k]) for k in range(PIECES)]
    copies.append(pltpu.make_async_copy(c, c_out, sems.at[PIECES]))
    for cp in copies:
        cp.start()
    for cp in copies:
        cp.wait()


def solution(mesh):
    def device_fn(h_init, c_init, w_rec, gate_bias):
        cells = H * W
        vm = pl.BlockSpec(memory_space=pltpu.VMEM)
        hbm = pl.BlockSpec(memory_space=pltpu.HBM)
        tile = pltpu.VMEM((BATCH, ROWS, PITCH, C), jnp.float32)
        strip = pltpu.VMEM((BATCH, 6, SROWS, C), jnp.float32)
        pack = pltpu.VMEM((2, BATCH, 2, PACK, C), jnp.float32)
        pair_sems = pltpu.SemaphoreType.DMA((2, BATCH, 2))
        hseq, clast = pl.pallas_call(
            kernel,
            out_shape=(jax.ShapeDtypeStruct((STEPS, BATCH, cells, C), jnp.bfloat16),
                       jax.ShapeDtypeStruct((BATCH, cells, C), jnp.float32)),
            in_specs=[hbm, hbm, hbm, hbm],
            out_specs=(vm, vm),
            scratch_shapes=[
                tile, tile, tile, strip, strip,
                pack, pack,
                pltpu.VMEM((4, 9 * C, C), jnp.bfloat16),
                pltpu.VMEM((BATCH, cells, C), jnp.bfloat16),
                pltpu.VMEM((STEPS, 4 * C), jnp.float32),
                pltpu.SemaphoreType.DMA((2, BATCH)),
                pltpu.SemaphoreType.DMA((2, BATCH)),
                pair_sems,
                pair_sems,
                pltpu.SemaphoreType.DMA((7,)),
            ],
            compiler_params=pltpu.CompilerParams(collective_id=0, has_side_effects=True, vmem_limit_bytes=26 << 20),
        )(*(pltpu.with_memory_space_constraint(v, pltpu.HBM) for v in (
            h_init.reshape(BATCH, cells, C), c_init.reshape(BATCH, cells, C), w_rec.reshape(9 * C, 4 * C), gate_bias)))
        anywhere = pl.BlockSpec(memory_space=pl.ANY)
        hseq, clast = pl.pallas_call(
            write_out,
            out_shape=(jax.ShapeDtypeStruct((STEPS, BATCH, cells, C), jnp.bfloat16),
                       jax.ShapeDtypeStruct((BATCH, cells, C), jnp.float32)),
            in_specs=[vm, vm],
            out_specs=(anywhere, anywhere),
            scratch_shapes=[pltpu.SemaphoreType.DMA((PIECES + 1,))],
            compiler_params=pltpu.CompilerParams(vmem_limit_bytes=26 << 20),
        )(hseq, clast)
        return hseq.reshape(STEPS, BATCH, H, W, C), clast.reshape(BATCH, H, W, C)

    state_spec = P("dp", "rows", "cols", None)
    return jax.shard_map(device_fn, mesh=mesh, in_specs=(state_spec, state_spec, P(), P()),
                         out_specs=(P(None, "dp", "rows", "cols", None), state_spec), check_vma=False)
```

```python
import jax
import jax.numpy as jnp
from jax import lax
from jax.experimental import pallas as pl
from jax.experimental.pallas import tpu as pltpu
from jax.sharding import PartitionSpec as P

MESH = pl.DeviceIdType.MESH
STEPS, BATCH, H, W, C = 24, 2, 32, 24, 128
PERIODS = STEPS // 2
RC = 8
NC = H // RC
M = RC * W
PITCH = 40
PAD = 8
ROWS = H + 2 * PAD
SP = 16
SROWS = H + 2 * SP
PACK = 3 * W + 8
CORNER = slice(3 * W, PACK)
PIECES = 11
A_ORDER = (0, 1, 2, 3)
B_ORDER = (0, 3, 1, 2)


def sigmoid(x):
    return 0.5 * jnp.tanh(0.5 * x) + 0.5


def places():
    row = lax.axis_index("rows")
    col = lax.axis_index("cols")
    nrow = lax.axis_size("rows")
    has = (row > 0, row < nrow - 1)
    halo_w = jnp.where(col == 0, 8 + W, 7)
    tap_plane = (jnp.where(col == 0, 0, 4), 3, jnp.where(col == 0, 4, 0))
    return has, halo_w, tap_plane


def flat(ref, b):
    return ref.at[b].reshape(ROWS * PITCH, C)


def strided(start, stride):
    return pl.ds(start, RC, stride)


def clear_borders(ref, b):
    for at in (0, 8 + W):
        ref[b, :, at:at + 8, :] = jnp.zeros((ROWS, 8, C), jnp.float32)


def run(units):
    held = None
    for unit in units + [None]:
        gate = unit[0]() if unit else None
        if held:
            held[0][1](held[1])
        held = (unit, gate) if unit else None


def make_units(he, st, hodd, c, bias, wt, precv, arrive, keep, put):
    has, halo_w, tap_plane = places()

    def gates(parts, t):
        lhs = jnp.concatenate(parts, axis=1)
        rhs = jnp.concatenate([wt[k] for k in range(4)], axis=1)
        return jnp.dot(lhs, rhs, preferred_element_type=jnp.float32)

    def update(gate, t, c_prev):
        gate = bias[pl.ds(t, 1), :] + gate
        c_next = sigmoid(gate[:, C:2 * C]) * c_prev + sigmoid(gate[:, :C]) * jnp.tanh(gate[:, 3 * C:])
        return (sigmoid(gate[:, 2 * C:3 * C]) * jnp.tanh(c_next)).astype(jnp.bfloat16), c_next

    def unit_a(s, b, i, t, seen):
        lo = i * RC - (1 if i == 0 else 0)
        n = RC + (1 if i in (0, NC - 1) else 0)
        wlo = i * RC - (RC if i == 0 else 0)
        wn = RC * (2 if i in (0, NC - 1) else 1)

        def dot():
            arrive(s, b, seen)
            parts = []
            for dh in range(3):
                for dw in range(3):
                    v = he[s][b, PAD + lo + dh - 1:PAD + lo + dh - 1 + n, 7 + dw:7 + dw + W, :].reshape(n * W, C)
                    r = st[s][b, tap_plane[dw], SP + wlo + dh - 1:SP + wlo + dh - 1 + wn, :]
                    v = jnp.concatenate([v, r, jnp.zeros((8, C), jnp.float32)], axis=0)
                    parts.append(v.astype(jnp.bfloat16))
            return gates(parts, t)

        def epilogue(gate):
            cm = c[b, i * M:(i + 1) * M, :]
            cw = st[s][b, 5, SP + wlo:SP + wlo + wn, :]
            z = jnp.zeros((8, C), jnp.float32)
            if i == 0:
                parts, m0 = [precv[s, b, 0, 2 * W:3 * W, :], cm, cw, z], W
            elif i == NC - 1:
                parts, m0 = [cm, precv[s, b, 1, 2 * W:3 * W, :], cw, z], 0
            else:
                parts, m0 = [cm, cw, z], 0
            h, c_next = update(gate, t, jnp.concatenate(parts, axis=0))
            c[b, i * M:(i + 1) * M, :] = c_next[m0:m0 + M]
            hf = h.astype(jnp.float32)
            main = hf[m0:m0 + M]
            keep(t, b, i, main.astype(jnp.bfloat16))
            hodd[b, PAD + i * RC:PAD + (i + 1) * RC, 8:8 + W, :] = main.reshape(RC, W, C)
            ring = hf[n * W:n * W + wn]
            f = flat(hodd, b)
            if i == 0:
                hodd[b, PAD - 1, 8:8 + W, :] = jnp.where(has[0], hf[:W], 0.0)
                f[strided(halo_w, PITCH), :] = jnp.where(has[0], ring[:RC], 0.0)
                f[strided(PAD * PITCH + halo_w, PITCH), :] = ring[RC:]
            elif i == NC - 1:
                hodd[b, PAD + H, 8:8 + W, :] = jnp.where(has[1], hf[M:M + W], 0.0)
                f[strided((PAD + i * RC) * PITCH + halo_w, PITCH), :] = ring[:RC]
                f[strided((PAD + H) * PITCH + halo_w, PITCH), :] = jnp.where(has[1], ring[RC:], 0.0)
            else:
                f[strided((PAD + i * RC) * PITCH + halo_w, PITCH), :] = ring

        return dot, epilogue

    def unit_b(n, b, i, t, send):
        def dot():
            parts = []
            for dh in range(3):
                for dw in range(3):
                    v = hodd[b, PAD + i * RC + dh - 1:PAD + (i + 1) * RC + dh - 1, 7 + dw:7 + dw + W, :]
                    parts.append(v.reshape(M, C).astype(jnp.bfloat16))
            return gates(parts, t)

        def epilogue(gate):
            h, c_next = update(gate, t, c[b, i * M:(i + 1) * M, :])
            c[b, i * M:(i + 1) * M, :] = c_next
            keep(t, b, i, h)
            put(n, b, i, h.astype(jnp.float32).reshape(RC, W, C), c_next, send)

        return dot, epilogue

    return unit_a, unit_b


def kernel(h0, c0, w, bias_in, hseq, c, hb, sb, precv, wt, bias, ha, hodd, sa, psend, hin,
           s_col, r_col, s_row, r_row, s_w):
    he = (ha, hb)
    st = (sa, sb)
    row = lax.axis_index("rows")
    col = lax.axis_index("cols")
    nrow = lax.axis_size("rows")
    up = lax.rem(row + nrow - 1, nrow)
    down = lax.rem(row + 1, nrow)
    side = 1 - col
    dev_side = {"cols": side}
    dev_row = ({"rows": up}, {"rows": down})
    dev_cor = ({"rows": up, "cols": side}, {"rows": down, "cols": side})

    has, halo_w, _ = places()
    edge_w = jnp.where(col == 0, 7 + W, 8)
    next_w = jnp.where(col == 0, 6 + W, 9)
    edge_c = jnp.where(col == 0, W - 1, 0)

    def remote(src, dst, ssem, rsem, dev):
        return pltpu.make_async_remote_copy(src, dst, ssem, rsem, device_id=dev, device_id_type=MESH)

    def col_copy(s, b, lo, n):
        rows = pl.ds(SP + lo, n)
        return remote(st[s].at[b, 0:3, rows, :], st[s].at[b, 3:6, rows, :], s_col.at[s, b], r_col.at[s, b], dev_side)

    def row_copy(s, b, d, part, dev):
        return remote(psend.at[s, b, d, part], precv.at[s, b, 1 - d, part], s_row.at[s, b, d], r_row.at[s, b, 1 - d], dev)

    def row_copies(s, b, d):
        return row_copy(s, b, d, CORNER, dev_cor[d]), row_copy(s, b, d, slice(0, 3 * W), dev_row[d])

    def put(s, b, i, h3, c2, send):
        if not send:
            return
        he[s][b, PAD + i * RC:PAD + (i + 1) * RC, 8:8 + W, :] = h3
        f = flat(he[s], b)
        base = (PAD + i * RC) * PITCH
        strip = (f[strided(base + edge_w, PITCH), :], f[strided(base + next_w, PITCH), :],
                 c.at[b][strided(i * M + edge_c, W), :])
        for k in range(3):
            st[s][b, k, SP + i * RC:SP + (i + 1) * RC, :] = strip[k]
        for d in range(2):
            if i == (0 if d == 0 else NC - 1):
                r = 0 if d == 0 else RC - 2
                q = 0 if d == 0 else (RC - 1) * W
                for k in range(3):
                    psend[s, b, d, 3 * W + 2 * k:3 * W + 2 * k + 2, :] = jnp.where(has[d], strip[k][r:r + 2], 0.0)
                psend[s, b, d, 0:2 * W, :] = jnp.where(has[d], h3[r:r + 2].reshape(2 * W, C), 0.0)
                psend[s, b, d, 2 * W:3 * W, :] = jnp.where(has[d], c2[q:q + W], 0.0)
                for cp in row_copies(s, b, d):
                    cp.start()
        col_copy(s, b, i * RC, RC).start()

    def insert(s, b, i):
        flat(he[s], b)[strided((PAD + i * RC) * PITCH + halo_w, PITCH), :] = st[s][b, 3, SP + i * RC:SP + (i + 1) * RC, :]

    def take_cols(s, b):
        cp = col_copy(s, b, 0, H)
        cp.wait_send()
        cp.wait_recv()
        for i in range(NC):
            insert(s, b, i)

    def take_row(s, b, d):
        row_copy(s, b, d, slice(0, PACK), dev_row[d]).wait_send()
        row_copy(s, b, 1 - d, slice(0, PACK), dev_row[d]).wait_recv()
        r = -2 if d == 0 else H
        he[s][b, PAD + r:PAD + r + 2, 8:8 + W, :] = precv[s, b, d, 0:2 * W, :].reshape(2, W, C)
        for k in range(3):
            st[s][b, 3 + k, SP + r:SP + r + 2, :] = precv[s, b, d, 3 * W + 2 * k:3 * W + 2 * k + 2, :]
        i = -1 if d == 0 else NC
        insert(s, b, i)
        st[s][b, 0, SP + i * RC:SP + (i + 1) * RC, :] = flat(he[s], b)[strided((PAD + i * RC) * PITCH + edge_w, PITCH), :]

    def arrive(s, b, seen):
        if not seen:
            seen.add(b)
            take_cols(s, b)
            for d in range(2):
                take_row(s, b, d)

    def keep(t, b, i, h):
        hseq[t, b, i * M:(i + 1) * M, :] = h

    unit_a, unit_b = make_units(he, st, hodd, c, bias, wt, precv, arrive, keep, put)

    def wave(s, b, p, send):
        seen = set()
        run([unit_a(s, b, i, 2 * p, seen) for i in A_ORDER] + [unit_b(1 - s, b, i, 2 * p + 1, send) for i in B_ORDER])

    def period(s, p):
        for b in range(BATCH):
            wave(s, b, p, True)

    load_state = [pltpu.make_async_copy(h0, hin, s_w.at[4]), pltpu.make_async_copy(c0, c, s_w.at[5])]
    load_w = [pltpu.make_async_copy(w.at[:, k * C:(k + 1) * C], wt.at[k], s_w.at[k]) for k in range(4)]
    load_w.append(pltpu.make_async_copy(bias_in, bias, s_w.at[6]))
    for cp in load_state + load_w:
        cp.start()
    for b in range(BATCH):
        for ref in (ha, hb, hodd):
            clear_borders(ref, b)
    barrier = pltpu.get_barrier_semaphore()
    for dev in (dev_side,) + dev_row + dev_cor:
        pl.semaphore_signal(barrier, inc=1, device_id=dev, device_id_type=MESH)
    for cp in load_state:
        cp.wait()
    pl.semaphore_wait(barrier, 5)
    for b in range(BATCH):
        for i in range(NC):
            h = hin[b, i * M:(i + 1) * M, :].astype(jnp.float32).reshape(RC, W, C)
            put(0, b, i, h, c[b, i * M:(i + 1) * M, :], True)
    for cp in load_w:
        cp.wait()

    def two(q, _):
        period(0, 2 * q)
        period(1, 2 * q + 1)
        return 0

    lax.fori_loop(0, PERIODS // 2 - 1, two, 0)
    period(0, PERIODS - 2)
    wave(1, 0, PERIODS - 1, False)
    arrive(1, 1, set())


def write_out(h, c, hb, sb, precv, wt, bias, h_out, c_out, hodd, c_new, h_new, sems):
    b, t0 = BATCH - 1, STEPS - 2
    n = t0 // PIECES
    pairs = [(h.at[k * n:(k + 1) * n], h_out.at[k * n:(k + 1) * n]) for k in range(PIECES)]
    pairs += [(h.at[t0:, 0:b], h_out.at[t0:, 0:b]), (c.at[0:b], c_out.at[0:b]),
              (h_new.at[0], h_out.at[t0, b]), (h_new.at[1], h_out.at[t0 + 1, b]), (c_new.at[b], c_out.at[b])]
    copies = [pltpu.make_async_copy(src, dst, sems.at[k]) for k, (src, dst) in enumerate(pairs)]
    for cp in copies[:-3]:
        cp.start()
    clear_borders(hodd, b)
    c_new[b] = c[b]

    def keep(t, b, i, v):
        h_new[t - t0, i * M:(i + 1) * M, :] = v

    nothing = lambda *_: None
    unit_a, unit_b = make_units((None, hb), (None, sb), hodd, c_new, bias, wt, precv, nothing, keep, nothing)
    run([unit_a(1, b, i, t0, None) for i in A_ORDER] + [unit_b(0, b, i, t0 + 1, False) for i in B_ORDER])
    for cp in copies[-3:]:
        cp.start()
    for cp in copies:
        cp.wait()


def solution(mesh):
    def device_fn(h_init, c_init, w_rec, gate_bias):
        cells = H * W
        vm = pl.BlockSpec(memory_space=pltpu.VMEM)
        hbm = pl.BlockSpec(memory_space=pltpu.HBM)
        tile = pltpu.VMEM((BATCH, ROWS, PITCH, C), jnp.float32)
        strip = pltpu.VMEM((BATCH, 6, SROWS, C), jnp.float32)
        pack = pltpu.VMEM((2, BATCH, 2, PACK, C), jnp.float32)
        pair_sems = pltpu.SemaphoreType.DMA((2, BATCH, 2))
        spec = lambda ref: jax.ShapeDtypeStruct(ref.shape, ref.dtype)
        results = (jax.ShapeDtypeStruct((STEPS, BATCH, cells, C), jnp.bfloat16),
                   jax.ShapeDtypeStruct((BATCH, cells, C), jnp.float32))
        weights = pltpu.VMEM((4, 9 * C, C), jnp.bfloat16)
        biases = pltpu.VMEM((STEPS, 4 * C), jnp.float32)
        held = pl.pallas_call(
            kernel,
            out_shape=results + tuple(spec(v) for v in (tile, strip, pack, weights, biases)),
            in_specs=[hbm] * 4,
            out_specs=(vm,) * 7,
            scratch_shapes=[
                tile, tile, strip, pack,
                pltpu.VMEM((BATCH, cells, C), jnp.bfloat16),
                pltpu.SemaphoreType.DMA((2, BATCH)),
                pltpu.SemaphoreType.DMA((2, BATCH)),
                pair_sems,
                pair_sems,
                pltpu.SemaphoreType.DMA((7,)),
            ],
            compiler_params=pltpu.CompilerParams(collective_id=0, has_side_effects=True, vmem_limit_bytes=26 << 20),
        )(*(pltpu.with_memory_space_constraint(v, pltpu.HBM) for v in (
            h_init.reshape(BATCH, cells, C), c_init.reshape(BATCH, cells, C), w_rec.reshape(9 * C, 4 * C), gate_bias)))
        hseq, clast = pl.pallas_call(
            write_out,
            out_shape=results,
            in_specs=[vm] * 7,
            out_specs=(pl.BlockSpec(memory_space=pl.ANY),) * 2,
            scratch_shapes=[
                tile,
                pltpu.VMEM((BATCH, cells, C), jnp.float32),
                pltpu.VMEM((2, cells, C), jnp.bfloat16),
                pltpu.SemaphoreType.DMA((PIECES + 5,)),
            ],
            compiler_params=pltpu.CompilerParams(vmem_limit_bytes=26 << 20),
        )(*held)
        return hseq.reshape(STEPS, BATCH, H, W, C), clast.reshape(BATCH, H, W, C)

    state_spec = P("dp", "rows", "cols", None)
    return jax.shard_map(device_fn, mesh=mesh, in_specs=(state_spec, state_spec, P(), P()),
                         out_specs=(P(None, "dp", "rows", "cols", None), state_spec), check_vma=False)
```

```python
import jax
import jax.numpy as jnp
from jax import lax
from jax.experimental import pallas as pl
from jax.experimental.pallas import tpu as pltpu
from jax.sharding import PartitionSpec as P

MESH = pl.DeviceIdType.MESH
STEPS, BATCH, H, W, C = 24, 2, 32, 24, 128
PERIODS = STEPS // 2
RC = 8
NC = H // RC
M = RC * W
PITCH = 40
PAD = 8
ROWS = H + 2 * PAD
SP = 16
SROWS = H + 2 * SP
PACK = 3 * W + 8
CORNER = slice(3 * W, PACK)
PIECES = 11
A_ORDER = (0, 1, 2, 3)
B_ORDER = (0, 3, 1, 2)


def sigmoid(x):
    return 0.5 * jnp.tanh(0.5 * x) + 0.5


def places():
    row = lax.axis_index("rows")
    col = lax.axis_index("cols")
    nrow = lax.axis_size("rows")
    has = (row > 0, row < nrow - 1)
    halo_w = jnp.where(col == 0, 8 + W, 7)
    tap_plane = (jnp.where(col == 0, 0, 4), 3, jnp.where(col == 0, 4, 0))
    return has, halo_w, tap_plane


def flat(ref, b):
    return ref.at[b].reshape(ROWS * PITCH, C)


def strided(start, stride):
    return pl.ds(start, RC, stride)


def clear_borders(ref, b):
    for at in (0, 8 + W):
        ref[b, :, at:at + 8, :] = jnp.zeros((ROWS, 8, C), jnp.float32)


def run(units):
    held = None
    for unit in units + [None]:
        gate = unit[0]() if unit else None
        if held:
            held[0][1](held[1])
        held = (unit, gate) if unit else None


def make_units(he, st, hodd, c, bias, wt, precv, arrive, keep, put):
    has, halo_w, tap_plane = places()

    def gates(parts, t):
        lhs = jnp.concatenate(parts, axis=1)
        rhs = jnp.concatenate([wt[k] for k in range(4)], axis=1)
        return jnp.dot(lhs, rhs, preferred_element_type=jnp.float32)

    def update(gate, t, c_prev):
        gate = bias[pl.ds(t, 1), :] + gate
        c_next = sigmoid(gate[:, C:2 * C]) * c_prev + sigmoid(gate[:, :C]) * jnp.tanh(gate[:, 3 * C:])
        return (sigmoid(gate[:, 2 * C:3 * C]) * jnp.tanh(c_next)).astype(jnp.bfloat16), c_next

    def unit_a(s, b, i, t, seen):
        lo = i * RC - (1 if i == 0 else 0)
        n = RC + (1 if i in (0, NC - 1) else 0)
        wlo = i * RC - (RC if i == 0 else 0)
        wn = RC * (2 if i in (0, NC - 1) else 1)

        def dot():
            arrive(s, b, seen)
            parts = []
            for dh in range(3):
                for dw in range(3):
                    v = he[s][b, PAD + lo + dh - 1:PAD + lo + dh - 1 + n, 7 + dw:7 + dw + W, :].reshape(n * W, C)
                    r = st[s][b, tap_plane[dw], SP + wlo + dh - 1:SP + wlo + dh - 1 + wn, :]
                    v = jnp.concatenate([v, r, jnp.zeros((8, C), jnp.float32)], axis=0)
                    parts.append(v.astype(jnp.bfloat16))
            return gates(parts, t)

        def epilogue(gate):
            cm = c[b, i * M:(i + 1) * M, :]
            cw = st[s][b, 5, SP + wlo:SP + wlo + wn, :]
            z = jnp.zeros((8, C), jnp.float32)
            if i == 0:
                parts, m0 = [precv[s, b, 0, 2 * W:3 * W, :], cm, cw, z], W
            elif i == NC - 1:
                parts, m0 = [cm, precv[s, b, 1, 2 * W:3 * W, :], cw, z], 0
            else:
                parts, m0 = [cm, cw, z], 0
            h, c_next = update(gate, t, jnp.concatenate(parts, axis=0))
            c[b, i * M:(i + 1) * M, :] = c_next[m0:m0 + M]
            hf = h.astype(jnp.float32)
            main = hf[m0:m0 + M]
            keep(t, b, i, main.astype(jnp.bfloat16))
            hodd[b, PAD + i * RC:PAD + (i + 1) * RC, 8:8 + W, :] = main.reshape(RC, W, C)
            ring = hf[n * W:n * W + wn]
            f = flat(hodd, b)
            if i == 0:
                hodd[b, PAD - 1, 8:8 + W, :] = jnp.where(has[0], hf[:W], 0.0)
                f[strided(halo_w, PITCH), :] = jnp.where(has[0], ring[:RC], 0.0)
                f[strided(PAD * PITCH + halo_w, PITCH), :] = ring[RC:]
            elif i == NC - 1:
                hodd[b, PAD + H, 8:8 + W, :] = jnp.where(has[1], hf[M:M + W], 0.0)
                f[strided((PAD + i * RC) * PITCH + halo_w, PITCH), :] = ring[:RC]
                f[strided((PAD + H) * PITCH + halo_w, PITCH), :] = jnp.where(has[1], ring[RC:], 0.0)
            else:
                f[strided((PAD + i * RC) * PITCH + halo_w, PITCH), :] = ring

        return dot, epilogue

    def unit_b(n, b, i, t, send):
        def dot():
            parts = []
            for dh in range(3):
                for dw in range(3):
                    v = hodd[b, PAD + i * RC + dh - 1:PAD + (i + 1) * RC + dh - 1, 7 + dw:7 + dw + W, :]
                    parts.append(v.reshape(M, C).astype(jnp.bfloat16))
            return gates(parts, t)

        def epilogue(gate):
            h, c_next = update(gate, t, c[b, i * M:(i + 1) * M, :])
            c[b, i * M:(i + 1) * M, :] = c_next
            keep(t, b, i, h)
            put(n, b, i, h.astype(jnp.float32).reshape(RC, W, C), c_next, send)

        return dot, epilogue

    return unit_a, unit_b


def kernel(h0, c0, w, bias_in, hseq, c, hb, sb, precv, wt, bias, ha, hodd, sa, psend, hin,
           s_col, r_col, s_row, r_row, s_w):
    he = (ha, hb)
    st = (sa, sb)
    row = lax.axis_index("rows")
    col = lax.axis_index("cols")
    nrow = lax.axis_size("rows")
    up = lax.rem(row + nrow - 1, nrow)
    down = lax.rem(row + 1, nrow)
    side = 1 - col
    dev_side = {"cols": side}
    dev_row = ({"rows": up}, {"rows": down})
    dev_cor = ({"rows": up, "cols": side}, {"rows": down, "cols": side})

    has, halo_w, _ = places()
    edge_w = jnp.where(col == 0, 7 + W, 8)
    next_w = jnp.where(col == 0, 6 + W, 9)
    edge_c = jnp.where(col == 0, W - 1, 0)

    def remote(src, dst, ssem, rsem, dev):
        return pltpu.make_async_remote_copy(src, dst, ssem, rsem, device_id=dev, device_id_type=MESH)

    def col_copy(s, b, lo, n):
        rows = pl.ds(SP + lo, n)
        return remote(st[s].at[b, 0:3, rows, :], st[s].at[b, 3:6, rows, :], s_col.at[s, b], r_col.at[s, b], dev_side)

    def row_copy(s, b, d, part, dev):
        return remote(psend.at[s, b, d, part], precv.at[s, b, 1 - d, part], s_row.at[s, b], r_row.at[s, b], dev)

    def row_copies(s, b, d):
        return row_copy(s, b, d, CORNER, dev_cor[d]), row_copy(s, b, d, slice(0, 3 * W), dev_row[d])

    def put(s, b, i, h3, c2, send):
        if not send:
            return
        he[s][b, PAD + i * RC:PAD + (i + 1) * RC, 8:8 + W, :] = h3
        f = flat(he[s], b)
        base = (PAD + i * RC) * PITCH
        strip = (f[strided(base + edge_w, PITCH), :], f[strided(base + next_w, PITCH), :],
                 c.at[b][strided(i * M + edge_c, W), :])
        for k in range(3):
            st[s][b, k, SP + i * RC:SP + (i + 1) * RC, :] = strip[k]
        for d in range(2):
            if i == (0 if d == 0 else NC - 1):
                r = 0 if d == 0 else RC - 2
                q = 0 if d == 0 else (RC - 1) * W
                for k in range(3):
                    psend[s, b, d, 3 * W + 2 * k:3 * W + 2 * k + 2, :] = jnp.where(has[d], strip[k][r:r + 2], 0.0)
                psend[s, b, d, 0:2 * W, :] = jnp.where(has[d], h3[r:r + 2].reshape(2 * W, C), 0.0)
                psend[s, b, d, 2 * W:3 * W, :] = jnp.where(has[d], c2[q:q + W], 0.0)
                for cp in row_copies(s, b, d):
                    cp.start()
        col_copy(s, b, i * RC, RC).start()

    def insert(s, b, i):
        flat(he[s], b)[strided((PAD + i * RC) * PITCH + halo_w, PITCH), :] = st[s][b, 3, SP + i * RC:SP + (i + 1) * RC, :]

    def take_cols(s, b):
        cp = col_copy(s, b, 0, H)
        cp.wait_send()
        cp.wait_recv()
        for i in range(NC):
            insert(s, b, i)

    def take_rows(s, b):
        cp = remote(psend.at[s, b], precv.at[s, b], s_row.at[s, b], r_row.at[s, b], dev_row[0])
        cp.wait_send()
        cp.wait_recv()
        for d in range(2):
            take_row(s, b, d)

    def take_row(s, b, d):
        r = -2 if d == 0 else H
        he[s][b, PAD + r:PAD + r + 2, 8:8 + W, :] = precv[s, b, d, 0:2 * W, :].reshape(2, W, C)
        for k in range(3):
            st[s][b, 3 + k, SP + r:SP + r + 2, :] = precv[s, b, d, 3 * W + 2 * k:3 * W + 2 * k + 2, :]
        i = -1 if d == 0 else NC
        insert(s, b, i)
        st[s][b, 0, SP + i * RC:SP + (i + 1) * RC, :] = flat(he[s], b)[strided((PAD + i * RC) * PITCH + edge_w, PITCH), :]

    def arrive(s, b, seen):
        if not seen:
            seen.add(b)
            take_cols(s, b)
            take_rows(s, b)

    def keep(t, b, i, h):
        hseq[t, b, i * M:(i + 1) * M, :] = h

    unit_a, unit_b = make_units(he, st, hodd, c, bias, wt, precv, arrive, keep, put)

    def wave(s, b, p, send):
        seen = set()
        run([unit_a(s, b, i, 2 * p, seen) for i in A_ORDER] + [unit_b(1 - s, b, i, 2 * p + 1, send) for i in B_ORDER])

    def period(s, p):
        for b in range(BATCH):
            wave(s, b, p, True)

    load_state = [pltpu.make_async_copy(h0, hin, s_w.at[4]), pltpu.make_async_copy(c0, c, s_w.at[5])]
    load_w = [pltpu.make_async_copy(w.at[:, k * C:(k + 1) * C], wt.at[k], s_w.at[k]) for k in range(4)]
    load_w.append(pltpu.make_async_copy(bias_in, bias, s_w.at[6]))
    for cp in load_state + load_w:
        cp.start()
    for b in range(BATCH):
        for ref in (ha, hb, hodd):
            clear_borders(ref, b)
    barrier = pltpu.get_barrier_semaphore()
    for dev in (dev_side,) + dev_row + dev_cor:
        pl.semaphore_signal(barrier, inc=1, device_id=dev, device_id_type=MESH)
    for cp in load_state:
        cp.wait()
    pl.semaphore_wait(barrier, 5)
    for b in range(BATCH):
        for i in range(NC):
            h = hin[b, i * M:(i + 1) * M, :].astype(jnp.float32).reshape(RC, W, C)
            put(0, b, i, h, c[b, i * M:(i + 1) * M, :], True)
    for cp in load_w:
        cp.wait()

    def two(q, _):
        period(0, 2 * q)
        period(1, 2 * q + 1)
        return 0

    lax.fori_loop(0, PERIODS // 2 - 1, two, 0)
    period(0, PERIODS - 2)
    wave(1, 0, PERIODS - 1, False)
    arrive(1, 1, set())


def write_out(h, c, hb, sb, precv, wt, bias, h_out, c_out, hodd, c_new, h_new, sems):
    b, t0 = BATCH - 1, STEPS - 2
    n = t0 // PIECES
    pairs = [(h.at[k * n:(k + 1) * n], h_out.at[k * n:(k + 1) * n]) for k in range(PIECES)]
    pairs += [(h.at[t0:, 0:b], h_out.at[t0:, 0:b]), (c.at[0:b], c_out.at[0:b]),
              (h_new.at[0], h_out.at[t0, b]), (h_new.at[1], h_out.at[t0 + 1, b]), (c_new.at[b], c_out.at[b])]
    copies = [pltpu.make_async_copy(src, dst, sems.at[k]) for k, (src, dst) in enumerate(pairs)]
    for cp in copies[:-3]:
        cp.start()
    clear_borders(hodd, b)
    c_new[b] = c[b]

    def keep(t, b, i, v):
        h_new[t - t0, i * M:(i + 1) * M, :] = v

    nothing = lambda *_: None
    unit_a, unit_b = make_units((None, hb), (None, sb), hodd, c_new, bias, wt, precv, nothing, keep, nothing)
    run([unit_a(1, b, i, t0, None) for i in A_ORDER] + [unit_b(0, b, i, t0 + 1, False) for i in B_ORDER])
    for cp in copies[-3:]:
        cp.start()
    for cp in copies:
        cp.wait()


def solution(mesh):
    def device_fn(h_init, c_init, w_rec, gate_bias):
        cells = H * W
        vm = pl.BlockSpec(memory_space=pltpu.VMEM)
        hbm = pl.BlockSpec(memory_space=pltpu.HBM)
        tile = pltpu.VMEM((BATCH, ROWS, PITCH, C), jnp.float32)
        strip = pltpu.VMEM((BATCH, 6, SROWS, C), jnp.float32)
        pack = pltpu.VMEM((2, BATCH, 2, PACK, C), jnp.float32)
        spec = lambda ref: jax.ShapeDtypeStruct(ref.shape, ref.dtype)
        results = (jax.ShapeDtypeStruct((STEPS, BATCH, cells, C), jnp.bfloat16),
                   jax.ShapeDtypeStruct((BATCH, cells, C), jnp.float32))
        weights = pltpu.VMEM((4, 9 * C, C), jnp.bfloat16)
        biases = pltpu.VMEM((STEPS, 4 * C), jnp.float32)
        held = pl.pallas_call(
            kernel,
            out_shape=results + tuple(spec(v) for v in (tile, strip, pack, weights, biases)),
            in_specs=[hbm] * 4,
            out_specs=(vm,) * 7,
            scratch_shapes=[
                tile, tile, strip, pack,
                pltpu.VMEM((BATCH, cells, C), jnp.bfloat16),
                pltpu.SemaphoreType.DMA((2, BATCH)),
                pltpu.SemaphoreType.DMA((2, BATCH)),
                pltpu.SemaphoreType.DMA((2, BATCH)),
                pltpu.SemaphoreType.DMA((2, BATCH)),
                pltpu.SemaphoreType.DMA((7,)),
            ],
            compiler_params=pltpu.CompilerParams(collective_id=0, has_side_effects=True, vmem_limit_bytes=26 << 20),
        )(*(pltpu.with_memory_space_constraint(v, pltpu.HBM) for v in (
            h_init.reshape(BATCH, cells, C), c_init.reshape(BATCH, cells, C), w_rec.reshape(9 * C, 4 * C), gate_bias)))
        hseq, clast = pl.pallas_call(
            write_out,
            out_shape=results,
            in_specs=[vm] * 7,
            out_specs=(pl.BlockSpec(memory_space=pl.ANY),) * 2,
            scratch_shapes=[
                tile,
                pltpu.VMEM((BATCH, cells, C), jnp.float32),
                pltpu.VMEM((2, cells, C), jnp.bfloat16),
                pltpu.SemaphoreType.DMA((PIECES + 5,)),
            ],
            compiler_params=pltpu.CompilerParams(vmem_limit_bytes=26 << 20),
        )(*held)
        return hseq.reshape(STEPS, BATCH, H, W, C), clast.reshape(BATCH, H, W, C)

    state_spec = P("dp", "rows", "cols", None)
    return jax.shard_map(device_fn, mesh=mesh, in_specs=(state_spec, state_spec, P(), P()),
                         out_specs=(P(None, "dp", "rows", "cols", None), state_spec), check_vma=False)
```
